32 devices in a mesh: groups: 2 (over x), blk: 4 (over y, core), col: 4 (over z).
Axes of the slice: x: 2, y: 2, z: 4, core: 2. Of those that a mesh axis runs over, the one named last changes fastest.
Arguments:
- pair_block: bfloat16 [4096, 16384], P(('groups', 'blk'), 'col'), parts along dimension 0, may hold values from -1.5 to 1.5
- occ_energy: float32 [2], P('groups'), parts along dimension 0, may hold values from -1.5 to -0.3
- virt_energy: float32 [4096], P('groups'), parts along dimension 0, may hold values from 0.2 to 3
- frequency: float32 [2], P('groups'), parts along dimension 0, may hold values from 0.2 to 2
Outputs:
- dielectric: float32 [32768, 16384], P(('groups', 'col'), 'blk'), parts along dimension 0
The draws below stay inside these ranges and needn't reach their ends.
There are 2 independent parts, one for each index of `groups`. The reference program is written for one: setup_inputs(seed, part) draws one part's arguments, and reference() takes and returns one part's arrays. A program takes and returns all parts, laid end to end along the dimension named above; each array names one. Nothing has to cross between parts.
All inputs are finite; a program needn't handle non-finite values.
Results may differ from the reference program's by a relative error of at most 0.0027.
Values may be sent and summed in bfloat16 or wider, within the bound.
A program may use at most 192 MiB of HBM per device.

```python
import math
import jax
import jax.numpy as jnp
from jax import lax

NAUX = 16384
NVIRT = 2048
NOCC = 1
NPAIR = 2048


def block_scale(rng, extent, split, low, largest):
    def one(dim, shards_of):
        steps = jax.random.uniform(jax.random.fold_in(jax.random.fold_in(rng, 6), dim), (shards_of,), jnp.float32, low / len(split), largest / len(split))
        return jnp.repeat(jnp.exp(steps), extent[dim] // shards_of).reshape((-1,) + (1,) * (len(extent) - dim - 1))

    level = one(*split[0])
    for cut in split[1:]:
        level = level * one(*cut)
    return level


def gaussian(own_key, shape, scale, limit, shards=(), held_as=jnp.bfloat16):
    values = scale * jax.random.normal(own_key, shape, jnp.float32)
    if shards:
        values = values * block_scale(own_key, shape, shards, -0.22, 0.18)
    return jnp.clip(values, -limit, limit).astype(held_as)


def setup_inputs(seed: int = 0, part: int = 0) -> dict:
    streams_of = jax.random.split(jax.random.key(seed), 5)
    part_splits = jax.random.split(jax.random.fold_in(streams_of[4], part), 5)
    pair_block = gaussian(part_splits[0], (NPAIR, NAUX), (0.7 * NPAIR ** -0.25), 1.5, ((0, 4), (1, 4)))
    occ_energy = jnp.clip(jax.random.uniform(part_splits[1], (NOCC,), jnp.float32, -1.5, -0.3), -1.5, -0.3)
    virt_energy = jnp.clip(jnp.exp(jax.random.uniform(part_splits[2], (NVIRT,), jnp.float32, math.log(0.2), math.log(3.0))), 0.2, 3.0)
    frequency = jnp.clip(jnp.exp(jax.random.uniform(part_splits[3], (1,), jnp.float32, math.log(0.2), math.log(2.0))), 0.2, 2.0)
    return {"pair_block": pair_block, "occ_energy": occ_energy, "virt_energy": virt_energy, "frequency": frequency}


def reference(pair_block, occ_energy, virt_energy, frequency):
    gap = (virt_energy[None, :] - occ_energy[:, None]).reshape(-1)
    weights = 2.0 * gap / (gap * gap + frequency[0] * frequency[0])
    scaled = (pair_block.astype(jnp.float32) * weights[:, None]).astype(jnp.bfloat16)
    return lax.dot_general(scaled, pair_block, (((0,), (0,)), ((), ())), preferred_element_type=jnp.float32)
```

```python
import functools

import jax
import jax.numpy as jnp
from jax import lax
from jax.experimental import pallas as pl
from jax.experimental.pallas import tpu as pltpu
from jax.sharding import PartitionSpec as P

MESH = pl.DeviceIdType.MESH
CHUNKS = 8
TO_Y, TO_SIB, FWD_SIB, ECHO, PART0, LOCAL0, ON_XB, LINE0, LINE1, CROSS0, CROSS1 = 0, 1, 2, 3, 4, 8, 12, 16, 17, 18, 19


def pair_weights(occ_energy, virt_energy, frequency):
    gap = (virt_energy[None, :] - occ_energy[:, None]).reshape(-1)
    return 2.0 * gap / (gap * gap + frequency[0] * frequency[0])


def gather_kernel(x_ref, xz, xb, tr, send, rz, rb, rt):
    rows = x_ref.shape[0]
    step_rows = rows // CHUNKS
    g, b, z = lax.axis_index("groups"), lax.axis_index("blk"), lax.axis_index("col")
    last = lax.axis_size("col") - 1
    y, k = b // 2, b % 2
    u, v = k + y - 2 * y * k, z + y * (last - 2 * z)
    tu, tv = 1 - u, last - v
    dz = 1 - 2 * y
    own, sib, opp, dia = b, 2 * y + 1 - k, 2 * (1 - y) + k, 2 * (1 - y) + 1 - k
    first = 2 * y + y
    second = 2 * y + 1 - y
    far0, far1 = 2 * (1 - y) + y, 2 * (1 - y) + 1 - y

    def at(ref, slot, j):
        return ref.at[pl.ds(pl.multiple_of(slot * rows + j * step_rows, step_rows), step_rows)]

    def copy(src, dst, ssem, rsem, dev):
        return pltpu.make_async_remote_copy(
            src_ref=src, dst_ref=dst, send_sem=ssem, recv_sem=rsem, device_id=(g, dev[0], dev[1]), device_id_type=MESH
        )

    def to(kind, j, src, ref, rsem, slot, dev, lane=0):
        return copy(src, at(ref, slot, j), send.at[kind + lane, j], rsem.at[slot, j], dev)

    def arrived(ref, rsem, slot, j):
        copy(at(ref, slot, j), at(ref, slot, j), send.at[0, j], rsem.at[slot, j], (sib, z)).wait_recv()

    source = v == u
    feeds_sib = v == 1 - u
    tz = -dz
    to_sib = (sib, z)
    hop1 = (b, z + dz * (1 - 2 * u))
    up = (b, z + dz)
    down = (b, z - dz)
    line = (b, z + tz)
    cross0, cross1 = (2 * (1 - y) + 1 - y, z), (2 * (1 - y) + y, z)

    def spread(j, src, shard, lane):
        yield source, to(PART0, j, src, xb, rb, shard, hop1, lane)
        yield feeds_sib, to(LOCAL0, j, src, xb, rb, shard, to_sib, lane)
        if lane < 2:
            yield (u == 1) & (v == 1), to(ON_XB, j, src, xb, rb, shard, up, lane)

    def own_sends(j):
        src = x_ref.at[pl.ds(pl.multiple_of(j * step_rows, step_rows), step_rows)]
        yield True, to(TO_SIB, j, src, xz, rz, own, to_sib)
        yield True, to(TO_Y, j, src, xz, rz, own, (opp, z))
        yield tv == 0, to(LINE0, j, src, tr, rt, 0, line)
        yield tv == 1, to(LINE1, j, src, tr, rt, 1, line)
        yield from spread(j, src, own, 0)

    def sib_sends(j):
        src = at(xz, sib, j)
        yield True, to(ECHO, j, src, xz, rz, sib, to_sib)
        yield from spread(j, src, sib, 1)

    def opp_sends(j):
        src = at(xz, opp, j)
        yield True, to(FWD_SIB, j, src, xz, rz, opp, to_sib)
        yield from spread(j, src, opp, 2)

    def dia_sends(j):
        yield from spread(j, at(xz, dia, j), dia, 3)

    passes = [
        (1, (tv == 1), tr, rt, 0, lambda j: to(LINE0, j, at(tr, 0, j), tr, rt, 0, line)),
        (1, (u == 0) & (v == 1), xb, rb, first, lambda j: to(ON_XB, j, at(xb, first, j), xb, rb, first, up, 0)),
        (2, (u == 1) & (v == 2), xb, rb, second, lambda j: to(ON_XB, j, at(xb, second, j), xb, rb, second, up, 0)),
        (2, (tv == 2), tr, rt, 1, lambda j: to(CROSS1, j, at(tr, 1, j), xb, rb, own, cross1)),
        (3, (u == 0) & (v == 2), xb, rb, first, lambda j: to(ON_XB, j, at(xb, first, j), xb, rb, first, up, 0)),
        (9, (u == 0) & (v == 1), xb, rb, second, lambda j: to(ON_XB, j, at(xb, second, j), xb, rb, second, up, 1)),
        (10, (u == 1) & (v == 2), xb, rb, first, lambda j: to(ON_XB, j, at(xb, first, j), xb, rb, first, up, 1)),
        (10, (tv == 2), tr, rt, 0, lambda j: to(LINE0, j, at(tr, 0, j), tr, rt, 0, line)),
        (11, (tv == 3), tr, rt, 0, lambda j: to(CROSS0, j, at(tr, 0, j), xb, rb, own, cross0)),
        (11, (u == 0) & (v == 2), xb, rb, second, lambda j: to(ON_XB, j, at(xb, second, j), xb, rb, second, up, 1)),
        (11, (u == 1) & (v == 2), xb, rb, far0, lambda j: to(ON_XB, j, at(xb, far0, j), xb, rb, far0, up, 2)),
        (11, (u == 1) & (v == 2), xb, rb, far1, lambda j: to(ON_XB, j, at(xb, far1, j), xb, rb, far1, up, 3)),
        (13, (u == 0) & (v == 3), xb, rb, far0, lambda j: to(ON_XB, j, at(xb, far0, j), xb, rb, far0, down, 2)),
        (13, (u == 0) & (v == 3), xb, rb, far1, lambda j: to(ON_XB, j, at(xb, far1, j), xb, rb, far1, down, 3)),
    ]

    def when(cond, f):
        if cond is True:
            f()
        else:
            pl.when(cond)(f)

    def start_all(sends):
        for cond, c in sends:
            when(cond, c.start)

    barrier = pltpu.get_barrier_semaphore()
    peers = [(sib, z), (opp, z), (dia, z)] + [(b, lax.rem(z + i, last + 1)) for i in range(1, last + 1)]
    for dev in peers:
        pl.semaphore_signal(barrier, inc=1, device_id=(g,) + dev, device_id_type=MESH)
    pl.semaphore_wait(barrier, len(peers))

    @pl.loop(0, CHUNKS)
    def _(j):
        start_all(own_sends(j))

    @pl.loop(0, CHUNKS)
    def _(j):
        arrived(xz, rz, sib, j)
        start_all(sib_sends(j))

    @pl.loop(0, CHUNKS + 13)
    def _(t):
        @pl.when(t < CHUNKS)
        def _():
            arrived(xz, rz, opp, t)
            start_all(opp_sends(t))

        @pl.when((t >= 1) & (t < CHUNKS + 1))
        def _():
            arrived(xz, rz, dia, t - 1)
            start_all(dia_sends(t - 1))

        for lag, role, ref, rsem, slot, send_on in passes:

            @pl.when(role & (t >= lag) & (t < lag + CHUNKS))
            def _():
                arrived(ref, rsem, slot, t - lag)
                send_on(t - lag).start()

    @pl.loop(0, CHUNKS)
    def _(j):
        arrived(xz, rz, own, j)
        near = ((u == 0) & (v == 1)) | (v == 2)
        far = ((u == 1) & (v == 2)) | ((u == 0) & (v == 3))

        @pl.when(jnp.logical_not(near))
        def _():
            arrived(xb, rb, first, j)
            arrived(xb, rb, second, j)

        @pl.when(jnp.logical_not(far))
        def _():
            arrived(xb, rb, far0, j)
            arrived(xb, rb, far1, j)

        for sends in (own_sends(j), sib_sends(j), opp_sends(j), dia_sends(j)):
            for cond, c in sends:
                when(cond, c.wait_send)
        for _, role, _, _, _, send_on in passes:
            pl.when(role)(send_on(j).wait_send)


def gather_both(pair_block):
    rows, cols = pair_block.shape
    full = jax.ShapeDtypeStruct((4 * rows, cols), pair_block.dtype)
    return pl.pallas_call(
        gather_kernel,
        out_shape=(full, full, jax.ShapeDtypeStruct((2 * rows, cols), pair_block.dtype)),
        in_specs=[pl.BlockSpec(memory_space=pl.ANY)],
        out_specs=[pl.BlockSpec(memory_space=pl.ANY)] * 3,
        scratch_shapes=[
            pltpu.SemaphoreType.DMA((20, CHUNKS)),
            pltpu.SemaphoreType.DMA((4, CHUNKS)),
            pltpu.SemaphoreType.DMA((4, CHUNKS)),
            pltpu.SemaphoreType.DMA((2, CHUNKS)),
        ],
        compiler_params=pltpu.CompilerParams(collective_id=0, has_side_effects=True),
    )(pair_block)


def shards(square, pair_block, occ_energy, virt_energy, frequency):
    weights = pair_weights(occ_energy, virt_energy, frequency)
    if square:
        own_columns, column_slab, _ = gather_both(pair_block)
    else:
        row_full = lax.all_gather(pair_block, "col", axis=1, tiled=True)
        column_slab = lax.all_to_all(row_full, "blk", split_axis=1, concat_axis=0, tiled=True)
        own_columns = lax.all_gather(pair_block, "blk", axis=0, tiled=True)
    scaled = (own_columns.astype(jnp.float32) * weights[:, None]).astype(jnp.bfloat16)
    return lax.dot_general(
        scaled, column_slab, (((0,), (0,)), ((), ())), preferred_element_type=jnp.float32
    )


def solution(mesh):
    square = mesh.shape["blk"] == 4 and mesh.shape["col"] == 4
    return jax.shard_map(
        functools.partial(shards, square),
        mesh=mesh,
        in_specs=(P(("groups", "blk"), "col"), P("groups"), P("groups"), P("groups")),
        out_specs=P(("groups", "col"), "blk"),
        check_vma=False,
    )
```
